32 devices in a mesh: cuts: 16 (over z, y, x), circ: 2 (over core).
Axes of the slice: x: 2, y: 2, z: 4, core: 2. Of those that a mesh axis runs over, the one named last changes fastest.
Arguments:
- sources: bfloat16 [16, 8, 2, 16, 1024], P('cuts', None, 'circ'), may hold values from -6 to 6
- block_inverse: bfloat16 [2, 1024, 1024], P('circ'), may hold values from -0.0115625 to 0.92
- memory_factor: float32 [16, 2, 1024], P('cuts', 'circ'), may hold values from 0.5 to 1
- coupling_target: int32 [2, 4], P('circ'), may hold values from 0 to 1, as said below
- coupling_weight: bfloat16 [2, 4, 128, 1024], P('circ'), may hold values from -0.09375 to 0.09375
- coarse_decay: float32 [16, 2, 1024], P('cuts', 'circ'), may hold values from 0.2 to 0.995
- initial_state: float32 [2, 16, 1024], P('circ'), may hold values from -6 to 6
Outputs:
- slice_starts: float32 [16, 2, 16, 1024], P('cuts', 'circ')
- waveform: bfloat16 [16, 8, 2, 16, 1024], P('cuts', None, 'circ')
The draws below stay inside these ranges and needn't reach their ends.
Inputs may be any that keep to these rules, and one draw needn't show every extreme that they name: `coupling_target`: row j names 4 subcircuits, j itself among them possibly; a row may name one subcircuit twice.
All inputs are finite; a program needn't handle non-finite values.
Results may differ from the reference program's by a relative error of at most 0.007.
Values sent between devices are 32-bit elements; how exact they have to be, the bound alone decides.
A program may use at most 64 MiB of HBM per device.

```python
import math
import jax
import jax.numpy as jnp
from jax import lax

CIRCUIT_NODES = 1024
PORTS = 128
SCEN = 16
STEPS = 8
SWEEPS = 3
ITERS = 2
KC = 4
SUB_DEV = 1
SUBCIRCUIT_COUNT = 2
TIME_SLICES = 16
N_CIRC = 2


def draw_block_inverse(key, part):
    key_diag = jax.random.fold_in(key, 11)
    key_off = jax.random.fold_in(key, 12)
    spread = 0.12 * CIRCUIT_NODES ** (-0.5)
    diagonal = jnp.exp(jax.random.uniform(key_diag, (SUBCIRCUIT_COUNT, CIRCUIT_NODES), jnp.float32, jnp.log(0.3), jnp.log(0.85)))
    offdiag = jnp.clip(jax.random.normal(key_off, (SUBCIRCUIT_COUNT, CIRCUIT_NODES, CIRCUIT_NODES), jnp.float32), -3.0, 3.0) * spread
    identity = jnp.eye(CIRCUIT_NODES, dtype=jnp.float32)
    return (offdiag + diagonal[:, :, None] * identity[None]).astype(jnp.bfloat16)


def draw_coupling_target(key, part):
    targets = jax.random.randint(jax.random.fold_in(key, 21), (SUBCIRCUIT_COUNT, KC), 0, SUBCIRCUIT_COUNT)
    return targets.astype(jnp.int32)


def draw_coarse_decay(key, part):
    random_key_list = [jax.random.fold_in(key, 31 + offset) for offset in range(5)]
    slow_share = 0.5
    slow_mask = jax.random.uniform(random_key_list[0], (SUBCIRCUIT_COUNT, CIRCUIT_NODES), jnp.float32) < slow_share
    sluggish_rate = jax.random.uniform(random_key_list[1], (TIME_SLICES, SUBCIRCUIT_COUNT, CIRCUIT_NODES), jnp.float32, 0.97, 0.995)
    fast_rate = jax.random.uniform(random_key_list[2], (TIME_SLICES, SUBCIRCUIT_COUNT, CIRCUIT_NODES), jnp.float32, 0.2, 0.6)
    spike_slices = jax.random.randint(random_key_list[3], (3,), 0, TIME_SLICES)
    spike_active = jnp.any(jnp.arange(TIME_SLICES)[:, None] == spike_slices[None, :], axis=1)
    spike_multiplier = jax.random.uniform(random_key_list[4], (TIME_SLICES, SUBCIRCUIT_COUNT, CIRCUIT_NODES), jnp.float32, 0.5, 0.8)
    sluggish_rate = jnp.where(spike_active[:, None, None], sluggish_rate * spike_multiplier, sluggish_rate)
    return jnp.where(slow_mask[None], sluggish_rate, fast_rate).astype(jnp.float32)


def level_of(key, dims, cuts, low, largest):
    def one(position, blocks):
        steps = jax.random.uniform(jax.random.fold_in(jax.random.fold_in(key, 6), position), (blocks,), jnp.float32, low / len(cuts), largest / len(cuts))
        return jnp.repeat(jnp.exp(steps), dims[position] // blocks).reshape((-1,) + (1,) * (len(dims) - position - 1))

    loudness = one(*cuts[0])
    for cut in cuts[1:]:
        loudness = loudness * one(*cut)
    return loudness


def normal_values(own_key, extent, deviation, most, pieces=(), held_as=jnp.bfloat16):
    array = jax.random.normal(own_key, extent, jnp.float32) * deviation
    if len(pieces) > 0:
        array = level_of(own_key, extent, pieces, -0.22, 0.18) * array
    return jnp.clip(array, min=-most, max=most).astype(held_as)


def setup_inputs(seed: int = 0) -> dict:
    streams_of = jax.random.split(jax.random.key(seed), 8)
    sources = normal_values(streams_of[0], (TIME_SLICES, STEPS, SUBCIRCUIT_COUNT, SCEN, CIRCUIT_NODES), 1.0, 6.0, ((0, 16), (2, 2)))
    block_inverse = draw_block_inverse(jax.random.fold_in(streams_of[7], 71), 0)
    memory_factor = jnp.clip(jnp.exp(math.log(1.0) - 0.6931472 * jax.random.uniform(streams_of[2], (TIME_SLICES, SUBCIRCUIT_COUNT, CIRCUIT_NODES), jnp.float32) ** level_of(streams_of[2], (TIME_SLICES, SUBCIRCUIT_COUNT, CIRCUIT_NODES), ((0, 16), (1, 2)), -0.2, 0.2)), 0.5, 1.0)
    coupling_target = draw_coupling_target(jax.random.fold_in(streams_of[7], 71), 0)
    coupling_weight = normal_values(streams_of[4], (SUBCIRCUIT_COUNT, KC, PORTS, CIRCUIT_NODES), (4 * CIRCUIT_NODES) ** -0.5, 0.09375, ((0, 2),))
    coarse_decay = draw_coarse_decay(jax.random.fold_in(streams_of[7], 71), 0)
    initial_state = normal_values(streams_of[6], (SUBCIRCUIT_COUNT, SCEN, CIRCUIT_NODES), 1.0, 6.0, ((0, 2),), jnp.float32)
    return {"sources": sources, "block_inverse": block_inverse, "memory_factor": memory_factor, "coupling_target": coupling_target, "coupling_weight": coupling_weight, "coarse_decay": coarse_decay, "initial_state": initial_state}


highest = lax.Precision.HIGHEST


def to_low(values):
    return lax.optimization_barrier(values.astype(jnp.bfloat16)).astype(jnp.float32)


def run_chain(decay_rate, coarse_terms, initial):
    def advance(carried, paired):
        rate_now, extra_term = paired
        return rate_now[:, None, :] * carried + extra_term, carried

    unused, starts = lax.scan(advance, initial, (decay_rate, coarse_terms))
    return starts


def coupling_inflow(wave_now, coupling_target, weights_wide):
    wave_low = to_low(wave_now)
    contrib = jnp.einsum('skpn,tsqn->sktqp', weights_wide, wave_low, precision=highest)
    owners = (coupling_target[:, :, None] == jnp.arange(SUBCIRCUIT_COUNT, dtype=jnp.int32)[None, None, :]).astype(jnp.float32)
    grouped = contrib.reshape((N_CIRC, SUB_DEV) + contrib.shape[1:])
    owner_groups = owners.reshape((N_CIRC, SUB_DEV) + owners.shape[1:])
    partial_sums = jnp.einsum('dskg,dsktqp->dgtqp', owner_groups, grouped, precision=highest)
    return jnp.sum(partial_sums, axis=0)


def fine_slice(begin_state, slice_sources, factor, block_wide, coupling_target, weights_wide):
    wave_now = jnp.broadcast_to(begin_state, (STEPS,) + begin_state.shape)
    for sweep_index in range(SWEEPS):
        inflow = coupling_inflow(wave_now, coupling_target, weights_wide)
        previous = begin_state
        columns = []
        for step_index in range(STEPS):
            drive_term = factor[:, None, :] * previous + slice_sources[step_index].astype(jnp.float32)
            drive_term = drive_term.at[:, :, :PORTS].add(inflow[:, step_index])
            previous = jnp.einsum('smn,sqn->sqm', block_wide, to_low(drive_term), precision=highest)
            columns.append(previous)
        wave_now = jnp.stack(columns)
    return wave_now


def reference(sources, block_inverse, memory_factor, coupling_target, coupling_weight, coarse_decay, initial_state):
    block_wide = block_inverse.astype(jnp.float32)
    weights_wide = coupling_weight.astype(jnp.float32)
    coarse_load = jnp.mean(sources.astype(jnp.float32), axis=1)
    begin_all = run_chain(coarse_decay, coarse_load, initial_state)
    waves = None
    for iteration in range(ITERS):
        def one_slice(packed):
            begin_state, slice_sources, factor = packed
            return fine_slice(begin_state, slice_sources, factor, block_wide, coupling_target, weights_wide)

        waves = lax.map(one_slice, (begin_all, sources, memory_factor))
        correction = waves[:, -1] - coarse_decay[:, :, None, :] * begin_all
        begin_all = run_chain(coarse_decay, correction, initial_state)
    return begin_all, waves.astype(jnp.bfloat16)
```

```python
import functools

import jax
import jax.numpy as jnp
from jax import lax
from jax.experimental import pallas as pl
from jax.experimental.pallas import tpu as pltpu
from jax.sharding import PartitionSpec as P

SWEEPS = 3
ITERS = 2
MESH = pl.DeviceIdType.MESH
F32 = jnp.float32
BF16 = jnp.bfloat16
SUB, LANE = 8, 128


def dot(a, b):
    return jnp.dot(a.astype(BF16), b.astype(BF16), preferred_element_type=F32)


def kernel(
    cuts,
    circ,
    steps,
    src_ref,
    inv_ref,
    mem_ref,
    tgt_ref,
    cw_ref,
    dec_ref,
    init_ref,
    start_ref,
    wave_ref,
    inv_t,
    pow1,
    pow2,
    pow4,
    port_t,
    resp,
    port_resp,
    own,
    free,
    terms_buf,
    gather_buf,
    chain_buf,
    state_buf,
    decay_buf,
    part_buf,
    inflow_buf,
    send1,
    recv1,
    send2,
    recv2,
    send_d,
    recv_d,
    send_x,
    recv_x,
):
    n = lax.axis_index("cuts")
    me = lax.axis_index("circ")
    nodes = inv_ref.shape[0]
    scen = init_ref.shape[0]
    rows = src_ref.shape[0]
    blocks, ports = cw_ref.shape[0], cw_ref.shape[1]
    cols = nodes // LANE
    pieces = (scen // SUB) * cols
    stride = cuts // pieces
    piece = n // stride
    owner = lax.rem(n, stride) == 0

    def cut(k):
        return lax.rem(n + k, cuts)

    def peer(k):
        return lax.rem(me + k, circ)

    barrier = pltpu.get_barrier_semaphore()

    @pl.loop(1, cuts)
    def _(k):
        pl.semaphore_signal(barrier, inc=1, device_id=(cut(k), me), device_id_type=MESH)

    for k in range(1, circ):
        pl.semaphore_signal(barrier, inc=1, device_id=(n, peer(k)), device_id_type=MESH)

    def tile(p):
        r, c = p // cols, p % cols
        return slice(r * SUB, (r + 1) * SUB), slice(c * LANE, (c + 1) * LANE)

    def term_copy(c, other, dest, source):
        return pltpu.make_async_remote_copy(
            src_ref=terms_buf.at[c, dest // stride],
            dst_ref=gather_buf.at[c, source],
            send_sem=send1.at[c, dest // stride],
            recv_sem=recv1.at[c, source],
            device_id=(other, me),
            device_id_type=MESH,
        )

    def decay_copy(other, dest, source):
        lane = pl.multiple_of(lax.rem(dest // stride, cols) * LANE, LANE)
        return pltpu.make_async_remote_copy(
            src_ref=dec_ref.at[:, pl.ds(lane, LANE)],
            dst_ref=decay_buf.at[source],
            send_sem=send_d.at[dest // stride],
            recv_sem=recv_d.at[source],
            device_id=(other, me),
            device_id_type=MESH,
        )

    def state_copy(c, other, dest, source_piece):
        return pltpu.make_async_remote_copy(
            src_ref=chain_buf.at[c, dest],
            dst_ref=state_buf.at[c, source_piece],
            send_sem=send2.at[c, dest],
            recv_sem=recv2.at[c, source_piece],
            device_id=(other, me),
            device_id_type=MESH,
        )

    def is_owner(d):
        return lax.rem(d, stride) == 0

    def chain_send(c, terms):
        for p in range(pieces):
            terms_buf[c, p] = terms[tile(p)]
        if c == 0:
            pl.semaphore_wait(barrier, cuts - 1 + circ - 1)

        @pl.loop(1, cuts)
        def _(k):
            d = cut(k)

            @pl.when(is_owner(d))
            def _():
                term_copy(c, d, d, n).start()
                if c == 0:
                    decay_copy(d, d, n).start()

    def chain_turn(c):
        @pl.when(owner)
        def _():
            if c == 0:
                lane = pl.multiple_of(lax.rem(piece, cols) * LANE, LANE)
                decay_buf[n] = dec_ref[:, pl.ds(lane, LANE)]
            gather_buf[c, n] = terms_buf[c, piece]

            @pl.loop(1, cuts)
            def _(k):
                s = cut(k)
                term_copy(c, s, n, s).wait_recv()
                if c == 0:
                    decay_copy(s, n, s).wait_recv()

            row = pl.multiple_of(piece // cols * SUB, SUB)
            lane = pl.multiple_of(lax.rem(piece, cols) * LANE, LANE)
            state = init_ref[pl.ds(row, SUB), pl.ds(lane, LANE)]
            for s in range(cuts):
                chain_buf[c, s] = state
                if s < cuts - 1:
                    state = decay_buf[s] * state + gather_buf[c, s]

            @pl.loop(1, cuts)
            def _(k):
                d = cut(k)
                state_copy(c, d, d, piece).start()

            state_buf[c, piece] = chain_buf[c, n]

    def chain_end(c):
        @pl.loop(1, cuts)
        def _(k):
            s = cut(k)

            @pl.when(is_owner(s))
            def _():
                state_copy(c, s, n, s // stride).wait_recv()

        return jnp.concatenate(
            [
                jnp.concatenate([state_buf[c, r * cols + q] for q in range(cols)], axis=1)
                for r in range(scen // SUB)
            ],
            axis=0,
        )

    def drain(c):
        @pl.loop(1, cuts)
        def _(k):
            d = cut(k)

            @pl.when(is_owner(d))
            def _():
                term_copy(c, d, d, n).wait_send()
                if c == 0:
                    decay_copy(d, d, n).wait_send()

            @pl.when(owner)
            def _():
                state_copy(c, d, d, piece).wait_send()

    def current_copy(e, height, k, source):
        return pltpu.make_async_remote_copy(
            src_ref=part_buf.at[e, peer(k), pl.ds(0, height)],
            dst_ref=inflow_buf.at[e, source, pl.ds(0, height)],
            send_sem=send_x.at[e, k - 1],
            recv_sem=recv_x.at[e, source],
            device_id=(n, peer(k)),
            device_id_type=MESH,
        )

    def exchange_start(e, partial):
        height = partial.shape[0]
        for g in range(circ):
            part_buf[e, g, 0:height] = partial[:, g * ports : (g + 1) * ports]
        for k in range(1, circ):
            current_copy(e, height, k, me).start()

    def exchange_end(e, height):
        total = part_buf[e, me, 0:height]
        for k in range(1, circ):
            current_copy(e, height, k, peer(k)).wait_recv()
            total = total + inflow_buf[e, peer(k), 0:height]
        return total

    def exchange_drain(e, height):
        for k in range(1, circ):
            current_copy(e, height, k, me).wait_send()

    wide = min(256, nodes)

    def product(out, left, right):
        @pl.loop(0, nodes, step=wide)
        def _(at):
            at = pl.multiple_of(at, wide)
            out[:, pl.ds(at, wide)] = dot(left[...], right[:, pl.ds(at, wide)]).astype(BF16)

    load = src_ref[0:scen].astype(F32)
    for t in range(1, steps):
        load = load + src_ref[t * scen : (t + 1) * scen].astype(F32)
    chain_send(0, load * (1.0 / steps))

    factor = jnp.broadcast_to(mem_ref[...], (LANE, nodes)).T
    for c in range(cols):
        at = slice(c * LANE, (c + 1) * LANE)
        turned = inv_ref[at, :].T
        inv_t[:, at] = turned
        pow1[:, at] = (turned.astype(F32) * factor).astype(BF16)
    product(pow2, pow1, pow1)
    own[...] = dot(src_ref[...], inv_t[...])
    own[scen:] = own[scen:] + dot(own[: rows - scen], pow1[...])

    chain_turn(0)

    product(pow4, pow2, pow2)
    span = 2
    for power in (pow2, pow4):
        if span < steps:
            own[span * scen :] = own[span * scen :] + dot(own[: rows - span * scen], power[...])
        span *= 2
    resp[0:ports] = inv_t[0:ports]
    resp[ports : 2 * ports] = dot(resp[0:ports], pow1[...]).astype(BF16)
    resp[2 * ports : 4 * ports] = dot(resp[0 : 2 * ports], pow2[...]).astype(BF16)
    resp[4 * ports : 8 * ports] = dot(resp[0 : 4 * ports], pow4[...]).astype(BF16)
    for g in range(circ):
        summed = jnp.zeros((ports, nodes), F32)
        for b in range(blocks):
            share = jnp.where(tgt_ref[0, b] == g, 1.0, 0.0).astype(F32)
            summed = summed + share * cw_ref[b].astype(F32)
        port_t[:, g * ports : (g + 1) * ports] = summed.astype(BF16).T
    port_resp[...] = dot(resp[...], port_t[...]).astype(BF16)

    def by_lag(currents):
        low = currents.astype(BF16)
        columns = [low]
        for lag in range(1, steps):
            columns.append(
                jnp.concatenate(
                    [jnp.zeros((lag * scen, ports), BF16), low[: rows - lag * scen]], axis=0
                )
            )
        return jnp.concatenate(columns, axis=1)

    begin = chain_end(0)
    last = rows - scen
    for iteration in range(ITERS):
        first = iteration * SWEEPS
        exchange_start(first, dot(begin, port_t[...]))
        v0 = begin.astype(BF16)
        v1 = dot(v0, pow1[...])
        v01 = jnp.concatenate([v0, v1.astype(BF16)], axis=0)
        v23 = dot(v01, pow2[...])
        v03 = jnp.concatenate([v01, v23.astype(BF16)], axis=0)
        v47 = dot(v03, pow4[...])
        v8 = dot(v47[0:scen], pow4[...])
        free[0:scen] = own[0:scen] + v1
        free[scen : 3 * scen] = own[scen : 3 * scen] + v23
        free[3 * scen : last] = own[3 * scen : last] + v47
        free[last:] = own[last:] + v8
        seen = dot(free[...], port_t[...])
        current = exchange_end(first, scen)
        current = jnp.concatenate([current] * steps, axis=0)
        for sweep in range(1, SWEEPS):
            exchange_start(first + sweep, seen + dot(by_lag(current), port_resp[...]))
            current = exchange_end(first + sweep, rows)
        lags = by_lag(current)
        if iteration < ITERS - 1:
            final = free[last:] + dot(lags[last:], resp[...])
        else:
            wave = free[...] + dot(lags, resp[...])
            wave_ref[...] = wave.astype(BF16)
            final = wave[last:]
        chain_send(iteration + 1, final - dec_ref[...] * begin)
        chain_turn(iteration + 1)
        begin = chain_end(iteration + 1)
    start_ref[...] = begin

    for c in range(ITERS + 1):
        drain(c)
    for e in range(SWEEPS * ITERS):
        exchange_drain(e, scen if e % SWEEPS == 0 else rows)


def solution(mesh):
    cuts, circ = mesh.shape["cuts"], mesh.shape["circ"]

    def shards(sources, inverse, memory, target, weight, decay, initial):
        steps, scen, nodes = sources.shape[1], sources.shape[3], sources.shape[4]
        blocks, ports = weight.shape[1], weight.shape[2]
        rows = steps * scen
        pieces = scen * nodes // (SUB * LANE)
        chains, swaps = ITERS + 1, ITERS * SWEEPS
        vmem = pl.BlockSpec(memory_space=pltpu.VMEM)
        smem = pl.BlockSpec(memory_space=pltpu.SMEM)
        dma = pltpu.SemaphoreType.DMA
        square = pltpu.VMEM((nodes, nodes), BF16)
        start, wave = pl.pallas_call(
            functools.partial(kernel, cuts, circ, steps),
            out_shape=(
                jax.ShapeDtypeStruct((scen, nodes), F32),
                jax.ShapeDtypeStruct((rows, nodes), BF16),
            ),
            in_specs=[vmem, vmem, vmem, smem, vmem, vmem, vmem],
            out_specs=(vmem, vmem),
            scratch_shapes=[
                square,
                square,
                square,
                square,
                pltpu.VMEM((nodes, circ * ports), BF16),
                pltpu.VMEM((steps * ports, nodes), BF16),
                pltpu.VMEM((steps * ports, circ * ports), BF16),
                pltpu.VMEM((rows, nodes), F32),
                pltpu.VMEM((rows, nodes), F32),
                pltpu.VMEM((chains, pieces, SUB, LANE), F32),
                pltpu.VMEM((chains, cuts, SUB, LANE), F32),
                pltpu.VMEM((chains, cuts, SUB, LANE), F32),
                pltpu.VMEM((chains, pieces, SUB, LANE), F32),
                pltpu.VMEM((cuts, 1, LANE), F32),
                pltpu.VMEM((swaps, circ, rows, ports), F32),
                pltpu.VMEM((swaps, circ, rows, ports), F32),
                dma((chains, pieces)),
                dma((chains, cuts)),
                dma((chains, cuts)),
                dma((chains, pieces)),
                dma((pieces,)),
                dma((cuts,)),
                dma((swaps, max(circ - 1, 1))),
                dma((swaps, circ)),
            ],
            compiler_params=pltpu.CompilerParams(
                collective_id=0, has_side_effects=True, vmem_limit_bytes=60 * 1024 * 1024
            ),
            name="parareal",
        )(
            sources.reshape(rows, nodes),
            inverse[0],
            memory.reshape(1, nodes),
            target,
            weight[0],
            decay.reshape(1, nodes),
            initial[0],
        )
        return start[None, None], wave.reshape(1, steps, 1, scen, nodes)

    return jax.shard_map(
        shards,
        mesh=mesh,
        in_specs=(
            P("cuts", None, "circ", None, None),
            P("circ", None, None),
            P("cuts", "circ", None),
            P("circ", None),
            P("circ", None, None, None),
            P("cuts", "circ", None),
            P("circ", None, None),
        ),
        out_specs=(P("cuts", "circ", None, None), P("cuts", None, "circ", None, None)),
        check_vma=False,
    )
```

```python
import functools

import jax
import jax.numpy as jnp
from jax import lax
from jax.experimental import pallas as pl
from jax.experimental.pallas import tpu as pltpu
from jax.sharding import PartitionSpec as P

SWEEPS = 3
ITERS = 2
MESH = pl.DeviceIdType.MESH
F32 = jnp.float32
BF16 = jnp.bfloat16
LANE = 128


def dot(a, b):
    return jnp.dot(a.astype(BF16), b.astype(BF16), preferred_element_type=F32)


def kernel(
    cuts,
    circ,
    steps,
    src_in,
    inv_in,
    mem_in,
    tgt_in,
    cw_in,
    dec_in,
    init_in,
    start_ref,
    wave_out,
    src_ref,
    inv_ref,
    mem_ref,
    tgt_ref,
    cw_ref,
    dec_ref,
    init_ref,
    wave_ref,
    sem_in,
    sem_out,
    inv_t,
    pow1,
    pow2,
    pow4,
    port_t,
    resp,
    port_resp,
    own,
    free,
    terms_buf,
    gather_buf,
    chain_buf,
    state_buf,
    decay_buf,
    part_buf,
    inflow_buf,
    send1,
    recv1,
    send2,
    recv2,
    send_d,
    recv_d,
    send_x,
    recv_x,
):
    n = lax.axis_index("cuts")
    me = lax.axis_index("circ")
    nodes = inv_ref.shape[0]
    scen = init_ref.shape[0]
    rows = src_ref.shape[0]
    blocks, ports = cw_ref.shape[0], cw_ref.shape[1]
    cols = nodes // LANE
    base = (cuts - cols) // 2
    piece = n - base
    owner = jnp.logical_and(n >= base, n < base + cols)
    lane = pl.multiple_of(piece * LANE, LANE)

    def cut(k):
        return lax.rem(n + k, cuts)

    def peer(k):
        return lax.rem(me + k, circ)

    barrier = pltpu.get_barrier_semaphore()

    @pl.loop(1, cuts)
    def _(k):
        pl.semaphore_signal(barrier, inc=1, device_id=(cut(k), me), device_id_type=MESH)

    for k in range(1, circ):
        pl.semaphore_signal(barrier, inc=1, device_id=(n, peer(k)), device_id_type=MESH)

    pairs = (
        (dec_in, dec_ref),
        (src_in, src_ref),
        (inv_in, inv_ref),
        (mem_in, mem_ref),
        (cw_in, cw_ref),
        (tgt_in, tgt_ref),
        (init_in, init_ref),
    )
    loads = [pltpu.make_async_copy(a, b, sem_in.at[k]) for k, (a, b) in enumerate(pairs)]
    for copy in loads:
        copy.start()

    def term_copy(c, k, dest, source):
        return pltpu.make_async_remote_copy(
            src_ref=terms_buf.at[c, k],
            dst_ref=gather_buf.at[c, source],
            send_sem=send1.at[c, k],
            recv_sem=recv1.at[c, source],
            device_id=(dest, me),
            device_id_type=MESH,
        )

    def decay_copy(k, dest, source):
        return pltpu.make_async_remote_copy(
            src_ref=dec_ref.at[:, pl.ds(k * LANE, LANE)],
            dst_ref=decay_buf.at[source],
            send_sem=send_d.at[k],
            recv_sem=recv_d.at[source],
            device_id=(dest, me),
            device_id_type=MESH,
        )

    def state_copy(c, dest, other, k):
        return pltpu.make_async_remote_copy(
            src_ref=chain_buf.at[c, dest],
            dst_ref=state_buf.at[c, k],
            send_sem=send2.at[c, dest],
            recv_sem=recv2.at[c, k],
            device_id=(other, me),
            device_id_type=MESH,
        )

    def sends_to(dest):
        return jnp.logical_and(n != dest, n < cuts - 1)

    def chain_send(c, terms):
        for k in range(cols):
            terms_buf[c, k] = terms[:, k * LANE : (k + 1) * LANE]
        for k in range(cols):

            @pl.when(sends_to(base + k))
            def _():
                term_copy(c, k, base + k, n).start()
                if c == 0:
                    decay_copy(k, base + k, n).start()

    def chain_turn(c):
        @pl.when(owner)
        def _():
            if c == 0:
                decay_buf[n] = dec_ref[:, pl.ds(lane, LANE)]
            gather_buf[c, n] = terms_buf[c, piece]
            state = init_ref[:, pl.ds(lane, LANE)]
            for s in range(cuts):
                chain_buf[c, s] = state

                @pl.when(n != s)
                def _():
                    state_copy(c, s, s, piece).start()
                    if s < cuts - 1:
                        term_copy(c, 0, s, s).wait_recv()
                        if c == 0:
                            decay_copy(0, s, s).wait_recv()

                if s < cuts - 1:
                    state = decay_buf[s] * state + gather_buf[c, s]
            state_buf[c, piece] = chain_buf[c, n]

    def chain_end(c):
        for k in range(cols):

            @pl.when(n != base + k)
            def _():
                state_copy(c, 0, base + k, k).wait_recv()

        return jnp.concatenate([state_buf[c, k] for k in range(cols)], axis=1)

    def drain(c):
        for k in range(cols):

            @pl.when(sends_to(base + k))
            def _():
                term_copy(c, k, base + k, n).wait_send()
                if c == 0:
                    decay_copy(k, base + k, n).wait_send()

        @pl.when(owner)
        def _():
            @pl.loop(1, cuts)
            def _(k):
                d = cut(k)
                state_copy(c, d, d, piece).wait_send()

    def current_copy(e, height, k, source):
        return pltpu.make_async_remote_copy(
            src_ref=part_buf.at[e, peer(k), pl.ds(0, height)],
            dst_ref=inflow_buf.at[e, source, pl.ds(0, height)],
            send_sem=send_x.at[e, k - 1],
            recv_sem=recv_x.at[e, source],
            device_id=(n, peer(k)),
            device_id_type=MESH,
        )

    def exchange_start(e, partial):
        height = partial.shape[0]
        for g in range(circ):
            part_buf[e, g, 0:height] = partial[:, g * ports : (g + 1) * ports]
        for k in range(1, circ):
            current_copy(e, height, k, me).start()

    def exchange_end(e, height):
        total = part_buf[e, me, 0:height]
        for k in range(1, circ):
            current_copy(e, height, k, peer(k)).wait_recv()
            total = total + inflow_buf[e, peer(k), 0:height]
        return total

    def exchange_drain(e, height):
        for k in range(1, circ):
            current_copy(e, height, k, me).wait_send()

    wide = min(256, nodes)

    def product(out, left, right):
        @pl.loop(0, nodes, step=wide)
        def _(at):
            at = pl.multiple_of(at, wide)
            out[:, pl.ds(at, wide)] = dot(left[...], right[:, pl.ds(at, wide)]).astype(BF16)

    for copy in loads[:4]:
        copy.wait()
    factor = jnp.broadcast_to(mem_ref[...], (LANE, nodes)).T
    for c in range(cols):
        at = slice(c * LANE, (c + 1) * LANE)
        turned = inv_ref[at, :].T
        inv_t[:, at] = turned
        pow1[:, at] = (turned.astype(F32) * factor).astype(BF16)
    for copy in loads[4:]:
        copy.wait()
    for g in range(circ):
        summed = jnp.zeros((ports, nodes), F32)
        for b in range(blocks):
            share = jnp.where(tgt_ref[0, b] == g, 1.0, 0.0).astype(F32)
            summed = summed + share * cw_ref[b].astype(F32)
        port_t[:, g * ports : (g + 1) * ports] = summed.astype(BF16).T

    load = src_ref[0:scen].astype(F32)
    for t in range(1, steps):
        load = load + src_ref[t * scen : (t + 1) * scen].astype(F32)
    pl.semaphore_wait(barrier, cuts - 1 + circ - 1)
    chain_send(0, load * (1.0 / steps))

    def one_step(values):
        exact = mem_ref[...] * values
        high = exact.astype(BF16)
        low = (exact - high.astype(F32)).astype(BF16)
        both = dot(jnp.concatenate([high, low], axis=0), inv_t[...])
        return both[: values.shape[0]] + both[values.shape[0] :]

    product(pow2, pow1, pow1)
    own[...] = dot(src_ref[...], inv_t[...])

    chain_turn(0)

    own[scen:] = own[scen:] + one_step(own[: rows - scen])
    product(pow4, pow2, pow2)
    span = 2
    for power in (pow2, pow4):
        if span < steps:
            own[span * scen :] = own[span * scen :] + dot(own[: rows - span * scen], power[...])
        span *= 2
    resp[0:ports] = inv_t[0:ports]
    resp[ports : 2 * ports] = dot(resp[0:ports], pow1[...]).astype(BF16)
    resp[2 * ports : 4 * ports] = dot(resp[0 : 2 * ports], pow2[...]).astype(BF16)
    resp[4 * ports : 8 * ports] = dot(resp[0 : 4 * ports], pow4[...]).astype(BF16)
    port_resp[...] = dot(resp[...], port_t[...]).astype(BF16)

    def by_lag(currents):
        low = currents.astype(BF16)
        columns = [low]
        for lag in range(1, steps):
            columns.append(
                jnp.concatenate(
                    [jnp.zeros((lag * scen, ports), BF16), low[: rows - lag * scen]], axis=0
                )
            )
        return jnp.concatenate(columns, axis=1)

    begin = chain_end(0)
    last = rows - scen
    for iteration in range(ITERS):
        first = iteration * SWEEPS
        exchange_start(first, dot(begin, port_t[...]))
        v0 = begin.astype(BF16)
        v1 = one_step(begin)
        v01 = jnp.concatenate([v0, v1.astype(BF16)], axis=0)
        v23 = dot(v01, pow2[...])
        v03 = jnp.concatenate([v01, v23.astype(BF16)], axis=0)
        v47 = dot(v03, pow4[...])
        v8 = dot(v47[0:scen], pow4[...])
        free[0:scen] = own[0:scen] + v1
        free[scen : 3 * scen] = own[scen : 3 * scen] + v23
        free[3 * scen : last] = own[3 * scen : last] + v47
        free[last:] = own[last:] + v8
        seen = dot(free[...], port_t[...])
        current = exchange_end(first, scen)
        current = jnp.concatenate([current] * steps, axis=0)
        for sweep in range(1, SWEEPS):
            exchange_start(first + sweep, seen + dot(by_lag(current), port_resp[...]))
            current = exchange_end(first + sweep, rows)
        lags = by_lag(current)
        if iteration < ITERS - 1:
            final = free[last:] + dot(lags[last:], resp[...])
        else:
            wave = free[...] + dot(lags, resp[...])
            wave_ref[...] = wave.astype(BF16)
            result = pltpu.make_async_copy(wave_ref, wave_out, sem_out)
            result.start()
            final = wave[last:]
        chain_send(iteration + 1, final - dec_ref[...] * begin)
        chain_turn(iteration + 1)
        begin = chain_end(iteration + 1)
    start_ref[...] = begin
    result.wait()

    for c in range(ITERS + 1):
        drain(c)
    for e in range(SWEEPS * ITERS):
        exchange_drain(e, scen if e % SWEEPS == 0 else rows)


def solution(mesh):
    cuts, circ = mesh.shape["cuts"], mesh.shape["circ"]

    def shards(sources, inverse, memory, target, weight, decay, initial):
        steps, scen, nodes = sources.shape[1], sources.shape[3], sources.shape[4]
        blocks, ports = weight.shape[1], weight.shape[2]
        rows = steps * scen
        cols = nodes // LANE
        chains, swaps = ITERS + 1, ITERS * SWEEPS
        vmem = pl.BlockSpec(memory_space=pltpu.VMEM)
        hbm = pl.BlockSpec(memory_space=pl.ANY)
        dma = pltpu.SemaphoreType.DMA
        square = pltpu.VMEM((nodes, nodes), BF16)
        start, wave = pl.pallas_call(
            functools.partial(kernel, cuts, circ, steps),
            out_shape=(
                jax.ShapeDtypeStruct((scen, nodes), F32),
                jax.ShapeDtypeStruct((rows, nodes), BF16),
            ),
            in_specs=[hbm] * 7,
            out_specs=(vmem, hbm),
            scratch_shapes=[
                pltpu.VMEM((rows, nodes), BF16),
                square,
                pltpu.VMEM((1, nodes), F32),
                pltpu.SMEM((1, blocks), jnp.int32),
                pltpu.VMEM((blocks, ports, nodes), BF16),
                pltpu.VMEM((1, nodes), F32),
                pltpu.VMEM((scen, nodes), F32),
                pltpu.VMEM((rows, nodes), BF16),
                dma((7,)),
                dma(()),
                square,
                square,
                square,
                square,
                pltpu.VMEM((nodes, circ * ports), BF16),
                pltpu.VMEM((steps * ports, nodes), BF16),
                pltpu.VMEM((steps * ports, circ * ports), BF16),
                pltpu.VMEM((rows, nodes), F32),
                pltpu.VMEM((rows, nodes), F32),
                pltpu.VMEM((chains, cols, scen, LANE), F32),
                pltpu.VMEM((chains, cuts, scen, LANE), F32),
                pltpu.VMEM((chains, cuts, scen, LANE), F32),
                pltpu.VMEM((chains, cols, scen, LANE), F32),
                pltpu.VMEM((cuts, 1, LANE), F32),
                pltpu.VMEM((swaps, circ, rows, ports), F32),
                pltpu.VMEM((swaps, circ, rows, ports), F32),
                dma((chains, cols)),
                dma((chains, cuts)),
                dma((chains, cuts)),
                dma((chains, cols)),
                dma((cols,)),
                dma((cuts,)),
                dma((swaps, max(circ - 1, 1))),
                dma((swaps, circ)),
            ],
            compiler_params=pltpu.CompilerParams(
                collective_id=0, has_side_effects=True, vmem_limit_bytes=60 * 1024 * 1024
            ),
            name="parareal",
        )(
            sources.reshape(rows, nodes),
            inverse[0],
            memory.reshape(1, nodes),
            target,
            weight[0],
            decay.reshape(1, nodes),
            initial[0],
        )
        return start[None, None], wave.reshape(1, steps, 1, scen, nodes)

    return jax.shard_map(
        shards,
        mesh=mesh,
        in_specs=(
            P("cuts", None, "circ", None, None),
            P("circ", None, None),
            P("cuts", "circ", None),
            P("circ", None),
            P("circ", None, None, None),
            P("cuts", "circ", None),
            P("circ", None, None),
        ),
        out_specs=(P("cuts", "circ", None, None), P("cuts", None, "circ", None, None)),
        check_vma=False,
    )
```

```python
import functools

import jax
import jax.numpy as jnp
from jax import lax
from jax.experimental import pallas as pl
from jax.experimental.pallas import tpu as pltpu
from jax.sharding import PartitionSpec as P

SWEEPS = 3
ITERS = 2
MESH = pl.DeviceIdType.MESH
F32 = jnp.float32
BF16 = jnp.bfloat16
LANE = 128


def dot(a, b):
    return jnp.dot(a.astype(BF16), b.astype(BF16), preferred_element_type=F32)


def kernel(
    cuts,
    circ,
    steps,
    src_in,
    inv_in,
    mem_in,
    tgt_in,
    cw_in,
    dec_in,
    init_in,
    start_ref,
    wave_out,
    src_ref,
    inv_ref,
    mem_ref,
    tgt_ref,
    cw_ref,
    dec_ref,
    init_ref,
    wave_ref,
    sem_in,
    sem_out,
    inv_t,
    pow1,
    pow2,
    pow4,
    port_t,
    resp,
    port_resp,
    own,
    free,
    terms_buf,
    gather_buf,
    chain_buf,
    state_buf,
    decay_buf,
    part_buf,
    inflow_buf,
    send1,
    recv1,
    send2,
    recv2,
    send_d,
    recv_d,
    send_x,
    recv_x,
):
    n = lax.axis_index("cuts")
    me = lax.axis_index("circ")
    nodes = inv_ref.shape[0]
    scen = init_ref.shape[0]
    rows = src_ref.shape[0]
    blocks, ports = cw_ref.shape[0], cw_ref.shape[1]
    cols = nodes // LANE
    base = (cuts - cols) // 2
    piece = n - base
    owner = jnp.logical_and(n >= base, n < base + cols)
    lane = pl.multiple_of(piece * LANE, LANE)

    def cut(k):
        return lax.rem(n + k, cuts)

    def peer(k):
        return lax.rem(me + k, circ)

    barrier = pltpu.get_barrier_semaphore()

    @pl.loop(1, cuts)
    def _(k):
        pl.semaphore_signal(barrier, inc=1, device_id=(cut(k), me), device_id_type=MESH)

    for k in range(1, circ):
        pl.semaphore_signal(barrier, inc=1, device_id=(n, peer(k)), device_id_type=MESH)

    pairs = (
        (dec_in, dec_ref),
        (src_in, src_ref),
        (inv_in, inv_ref),
        (mem_in, mem_ref),
        (cw_in, cw_ref),
        (tgt_in, tgt_ref),
        (init_in, init_ref),
    )
    loads = [pltpu.make_async_copy(a, b, sem_in.at[k]) for k, (a, b) in enumerate(pairs)]
    for copy in loads:
        copy.start()

    def term_copy(c, k, dest, source):
        return pltpu.make_async_remote_copy(
            src_ref=terms_buf.at[c, k],
            dst_ref=gather_buf.at[c, source],
            send_sem=send1.at[c, k],
            recv_sem=recv1.at[c, source],
            device_id=(dest, me),
            device_id_type=MESH,
        )

    def decay_copy(k, dest, source):
        return pltpu.make_async_remote_copy(
            src_ref=dec_ref.at[:, pl.ds(k * LANE, LANE)],
            dst_ref=decay_buf.at[source],
            send_sem=send_d.at[k],
            recv_sem=recv_d.at[source],
            device_id=(dest, me),
            device_id_type=MESH,
        )

    def state_copy(c, dest, other, k):
        return pltpu.make_async_remote_copy(
            src_ref=chain_buf.at[c, dest],
            dst_ref=state_buf.at[c, k],
            send_sem=send2.at[c, dest],
            recv_sem=recv2.at[c, k],
            device_id=(other, me),
            device_id_type=MESH,
        )

    def sends_to(dest):
        return jnp.logical_and(n != dest, n < cuts - 1)

    def chain_send(c, terms):
        for k in range(cols):
            terms_buf[c, k] = terms[:, k * LANE : (k + 1) * LANE]
        for k in range(cols):

            @pl.when(sends_to(base + k))
            def _():
                term_copy(c, k, base + k, n).start()
                if c == 0:
                    decay_copy(k, base + k, n).start()

    def chain_turn(c):
        @pl.when(owner)
        def _():
            if c == 0:
                decay_buf[n] = dec_ref[:, pl.ds(lane, LANE)]
            gather_buf[c, n] = terms_buf[c, piece]
            state = init_ref[:, pl.ds(lane, LANE)]
            for s in range(cuts):
                chain_buf[c, s] = state

                @pl.when(n != s)
                def _():
                    state_copy(c, s, s, piece).start()
                    if s < cuts - 1:
                        term_copy(c, 0, s, s).wait_recv()
                        if c == 0:
                            decay_copy(0, s, s).wait_recv()

                if s < cuts - 1:
                    state = decay_buf[s] * state + gather_buf[c, s]
            state_buf[c, piece] = chain_buf[c, n]

    def chain_end(c):
        for k in range(cols):

            @pl.when(n != base + k)
            def _():
                state_copy(c, 0, base + k, k).wait_recv()

        return jnp.concatenate([state_buf[c, k] for k in range(cols)], axis=1)

    def drain(c):
        for k in range(cols):

            @pl.when(sends_to(base + k))
            def _():
                term_copy(c, k, base + k, n).wait_send()
                if c == 0:
                    decay_copy(k, base + k, n).wait_send()

        @pl.when(owner)
        def _():
            @pl.loop(1, cuts)
            def _(k):
                d = cut(k)
                state_copy(c, d, d, piece).wait_send()

    def current_copy(e, height, k, source):
        return pltpu.make_async_remote_copy(
            src_ref=part_buf.at[e, peer(k), pl.ds(0, height)],
            dst_ref=inflow_buf.at[e, source, pl.ds(0, height)],
            send_sem=send_x.at[e, k - 1],
            recv_sem=recv_x.at[e, source],
            device_id=(n, peer(k)),
            device_id_type=MESH,
        )

    def exchange_start(e, partial):
        height = partial.shape[0]
        for g in range(circ):
            part_buf[e, g, 0:height] = partial[:, g * ports : (g + 1) * ports]
        for k in range(1, circ):
            current_copy(e, height, k, me).start()

    def exchange_end(e, height):
        total = part_buf[e, me, 0:height]
        for k in range(1, circ):
            current_copy(e, height, k, peer(k)).wait_recv()
            total = total + inflow_buf[e, peer(k), 0:height]
        return total

    def exchange_drain(e, height):
        for k in range(1, circ):
            current_copy(e, height, k, me).wait_send()

    wide = min(256, nodes)

    def product(out, left, right):
        @pl.loop(0, nodes, step=wide)
        def _(at):
            at = pl.multiple_of(at, wide)
            out[:, pl.ds(at, wide)] = dot(left[...], right[:, pl.ds(at, wide)]).astype(BF16)

    for copy in loads[:4]:
        copy.wait()
    factor = jnp.broadcast_to(mem_ref[...], (LANE, nodes)).T
    for c in range(cols):
        at = slice(c * LANE, (c + 1) * LANE)
        turned = inv_ref[at, :].T
        inv_t[:, at] = turned
        pow1[:, at] = (turned.astype(F32) * factor).astype(BF16)
    for copy in loads[4:]:
        copy.wait()
    for g in range(circ):
        summed = jnp.zeros((ports, nodes), F32)
        for b in range(blocks):
            share = jnp.where(tgt_ref[0, b] == g, 1.0, 0.0).astype(F32)
            summed = summed + share * cw_ref[b].astype(F32)
        port_t[:, g * ports : (g + 1) * ports] = summed.astype(BF16).T

    load = src_ref[0:scen].astype(F32)
    for t in range(1, steps):
        load = load + src_ref[t * scen : (t + 1) * scen].astype(F32)
    pl.semaphore_wait(barrier, cuts - 1 + circ - 1)
    chain_send(0, load * (1.0 / steps))

    def one_step(values):
        exact = mem_ref[...] * values
        high = exact.astype(BF16)
        low = (exact - high.astype(F32)).astype(BF16)
        both = dot(jnp.concatenate([high, low], axis=0), inv_t[...])
        return both[: values.shape[0]] + both[values.shape[0] :]

    product(pow2, pow1, pow1)
    own[...] = dot(src_ref[...], inv_t[...])

    chain_turn(0)

    own[scen:] = own[scen:] + one_step(own[: rows - scen])
    product(pow4, pow2, pow2)
    span = 2
    for power in (pow2, pow4):
        if span < steps:
            own[span * scen :] = own[span * scen :] + dot(own[: rows - span * scen], power[...])
        span *= 2
    resp[0:ports] = inv_t[0:ports]
    resp[ports : 2 * ports] = dot(resp[0:ports], pow1[...]).astype(BF16)
    resp[2 * ports : 4 * ports] = dot(resp[0 : 2 * ports], pow2[...]).astype(BF16)
    resp[4 * ports : 8 * ports] = dot(resp[0 : 4 * ports], pow4[...]).astype(BF16)
    port_resp[...] = dot(resp[...], port_t[...]).astype(BF16)

    def by_lag(currents):
        low = currents.astype(BF16)
        columns = [low]
        for lag in range(1, steps):
            columns.append(
                jnp.concatenate(
                    [jnp.zeros((lag * scen, ports), BF16), low[: rows - lag * scen]], axis=0
                )
            )
        return jnp.concatenate(columns, axis=1)

    begin = chain_end(0)
    last = rows - scen
    for iteration in range(ITERS):
        first = iteration * SWEEPS
        exchange_start(first, dot(begin, port_t[...]))
        v0 = begin.astype(BF16)
        v1 = one_step(begin)
        v01 = jnp.concatenate([v0, v1.astype(BF16)], axis=0)
        v23 = dot(v01, pow2[...])
        v03 = jnp.concatenate([v01, v23.astype(BF16)], axis=0)
        v47 = dot(v03, pow4[...])
        v8 = dot(v47[0:scen], pow4[...])
        free[0:scen] = own[0:scen] + v1
        free[scen : 3 * scen] = own[scen : 3 * scen] + v23
        free[3 * scen : last] = own[3 * scen : last] + v47
        free[last:] = own[last:] + v8
        seen = dot(free[...], port_t[...])
        current = exchange_end(first, scen)
        current = jnp.concatenate([current] * steps, axis=0)
        for sweep in range(1, SWEEPS):
            exchange_start(first + sweep, seen + dot(by_lag(current), port_resp[...]))
            current = exchange_end(first + sweep, rows)
        lags = by_lag(current)
        if iteration < ITERS - 1:
            final = free[last:] + dot(lags[last:], resp[...])
        else:
            wave = free[...] + dot(lags, resp[...])
            wave_ref[...] = wave.astype(BF16)
            result = pltpu.make_async_copy(wave_ref, wave_out, sem_out)
            result.start()
            final = wave[last:]
        chain_send(iteration + 1, final - dec_ref[...] * begin)
        chain_turn(iteration + 1)
        begin = chain_end(iteration + 1)
    start_ref[...] = begin
    result.wait()

    for c in range(ITERS + 1):
        drain(c)
    for e in range(SWEEPS * ITERS):
        exchange_drain(e, scen if e % SWEEPS == 0 else rows)


def hand_over(start_in, wave_in, start_out, wave_out):
    start_out[...] = start_in[...]
    wave_out[...] = wave_in[...]


def solution(mesh):
    cuts, circ = mesh.shape["cuts"], mesh.shape["circ"]

    def shards(sources, inverse, memory, target, weight, decay, initial):
        steps, scen, nodes = sources.shape[1], sources.shape[3], sources.shape[4]
        blocks, ports = weight.shape[1], weight.shape[2]
        rows = steps * scen
        cols = nodes // LANE
        chains, swaps = ITERS + 1, ITERS * SWEEPS
        vmem = pl.BlockSpec(memory_space=pltpu.VMEM)
        hbm = pl.BlockSpec(memory_space=pl.ANY)
        dma = pltpu.SemaphoreType.DMA
        square = pltpu.VMEM((nodes, nodes), BF16)
        start, wave = pl.pallas_call(
            functools.partial(kernel, cuts, circ, steps),
            out_shape=(
                jax.ShapeDtypeStruct((scen, nodes), F32),
                jax.ShapeDtypeStruct((rows, nodes), BF16),
            ),
            in_specs=[hbm] * 7,
            out_specs=(vmem, hbm),
            scratch_shapes=[
                pltpu.VMEM((rows, nodes), BF16),
                square,
                pltpu.VMEM((1, nodes), F32),
                pltpu.SMEM((1, blocks), jnp.int32),
                pltpu.VMEM((blocks, ports, nodes), BF16),
                pltpu.VMEM((1, nodes), F32),
                pltpu.VMEM((scen, nodes), F32),
                pltpu.VMEM((rows, nodes), BF16),
                dma((7,)),
                dma(()),
                square,
                square,
                square,
                square,
                pltpu.VMEM((nodes, circ * ports), BF16),
                pltpu.VMEM((steps * ports, nodes), BF16),
                pltpu.VMEM((steps * ports, circ * ports), BF16),
                pltpu.VMEM((rows, nodes), F32),
                pltpu.VMEM((rows, nodes), F32),
                pltpu.VMEM((chains, cols, scen, LANE), F32),
                pltpu.VMEM((chains, cuts, scen, LANE), F32),
                pltpu.VMEM((chains, cuts, scen, LANE), F32),
                pltpu.VMEM((chains, cols, scen, LANE), F32),
                pltpu.VMEM((cuts, 1, LANE), F32),
                pltpu.VMEM((swaps, circ, rows, ports), F32),
                pltpu.VMEM((swaps, circ, rows, ports), F32),
                dma((chains, cols)),
                dma((chains, cuts)),
                dma((chains, cuts)),
                dma((chains, cols)),
                dma((cols,)),
                dma((cuts,)),
                dma((swaps, max(circ - 1, 1))),
                dma((swaps, circ)),
            ],
            compiler_params=pltpu.CompilerParams(
                collective_id=0, has_side_effects=True, vmem_limit_bytes=60 * 1024 * 1024
            ),
            name="parareal",
        )(
            sources.reshape(rows, nodes),
            inverse[0],
            memory.reshape(1, nodes),
            target,
            weight[0],
            decay.reshape(1, nodes),
            initial[0],
        )
        start, wave = pl.pallas_call(
            hand_over,
            out_shape=(
                jax.ShapeDtypeStruct(start.shape, F32),
                jax.ShapeDtypeStruct(wave.shape, BF16),
            ),
            in_specs=[vmem, vmem],
            out_specs=(vmem, vmem),
            name="hand_over",
        )(start, wave)
        return start[None, None], wave.reshape(1, steps, 1, scen, nodes)

    return jax.shard_map(
        shards,
        mesh=mesh,
        in_specs=(
            P("cuts", None, "circ", None, None),
            P("circ", None, None),
            P("cuts", "circ", None),
            P("circ", None),
            P("circ", None, None, None),
            P("cuts", "circ", None),
            P("circ", None, None),
        ),
        out_specs=(P("cuts", "circ", None, None), P("cuts", None, "circ", None, None)),
        check_vma=False,
    )
```
